32 devices in a mesh: row: 4 (over z), col: 8 (over y, x, core).
Axes of the slice: x: 2, y: 2, z: 4, core: 2. Of those that a mesh axis runs over, the one named last changes fastest.
Arguments:
- points: float32 [16, 32768], P(None, ('row', 'col')), may hold values from -6 to 6
- inverse_scales: float32 [16], replicated, may hold values from 0.05 to 31.255105
- probe_signs: int32 [32768, 128], P(('row', 'col')), may hold values 0 or 1
Outputs:
- trace_terms: float32 [128], replicated
- logdet_terms: float32 [128], replicated
The draws below stay inside these ranges and needn't reach their ends.
All inputs are finite; a program needn't handle non-finite values. No bound on the sum of `probe_signs` on one device may be relied on, other than what follows from the above.
Results may differ from the reference program's by a relative error of at most 0.0014.
Values may be sent and summed in bfloat16 or wider, within the bound.
A program may use at most 128 MiB of HBM per device.

```python
import math
import jax
import jax.numpy as jnp
from jax import lax

N = 32768
DIM = 16
PROBES = 128
STEPS = 3


def cluster_table(key):
    level_key, slot_key = jax.random.split(jax.random.fold_in(key, 29))
    positions = jnp.arange(N, dtype=jnp.int32)
    level_draw = jax.random.randint(level_key, (N,), 0, 6)
    levels = jnp.minimum(level_draw, 3)
    block_sizes = [max(N // 128, 1), max(N // 32, 1), max(N // 8, 1), N]
    counts = [max(block_sizes[0] // 60, 1), max(block_sizes[1] // 60, 1), max(block_sizes[2] // 60, 1), max(N // 20, 1)]
    raw_slots = jax.random.randint(slot_key, (N,), 0, 1 << 20)
    table_rows = jnp.zeros((N,), jnp.int32)
    for level_num in range(4):
        slot_ids = raw_slots % counts[level_num]
        candidate = level_num * N + positions // block_sizes[level_num] * counts[level_num] + slot_ids
        table_rows = jnp.where(levels == level_num, candidate, table_rows)
    return table_rows.astype(jnp.int32)


def draw_points(key, part):
    table_rows = cluster_table(key)
    centre_key, jitter_key = jax.random.split(jax.random.fold_in(key, 41))
    centres = jax.random.normal(centre_key, (DIM, 4 * N), jnp.float32)
    jitter = 0.5 * jax.random.normal(jitter_key, (DIM, N), jnp.float32)
    return jnp.clip(centres[:, table_rows] + jitter, -6.0, 6.0)


def draw_inverse_scales(key, part):
    second_key = jax.random.fold_in(jax.random.fold_in(key, 17), 1)
    return jnp.exp(jax.random.uniform(second_key, (DIM,), jnp.float32, math.log(0.25), math.log(0.5)))


def touch_ends(array, stream_key, low, largest):
    longest = array.shape.index(max(array.shape))
    spots = []
    for shift in (0, 1):
        where = [jax.random.randint(jax.random.fold_in(stream_key, axis), (), 0, length) for axis, length in enumerate(array.shape)]
        where[longest] = (where[longest] + shift) % array.shape[longest]
        spots.append(tuple(where))
    return array.at[spots[0]].set(low).at[spots[1]].set(largest)


def setup_inputs(seed: int = 0) -> dict:
    key_of = jax.random.split(jax.random.key(seed), 4)
    points = draw_points(jax.random.fold_in(key_of[3], 71), 0)
    inverse_scales = draw_inverse_scales(jax.random.fold_in(key_of[3], 71), 0)
    probe_signs = touch_ends((jax.random.randint(key_of[2], (N, PROBES), 0, 2) < 1).astype(jnp.int32), jax.random.fold_in(key_of[2], 1), 0, 1)
    return {"points": points, "inverse_scales": inverse_scales, "probe_signs": probe_signs}


epsilon = 1e-06
noise_level = 1.0
jacobi_sweeps = 6

def kernel_block(left_points, right_points):
    cross_term = lax.dot_general(left_points, right_points, (((0,), (0,)), ((), ())), precision=lax.Precision.HIGHEST, preferred_element_type=jnp.float32)
    left_norms = lax.optimization_barrier(jnp.sum(left_points * left_points, axis=0))
    right_norms = lax.optimization_barrier(jnp.sum(right_points * right_points, axis=0))
    distance = jnp.maximum(left_norms[:, None] + right_norms[None, :] - 2.0 * cross_term, 0.0)
    return jnp.exp(-0.5 * distance).astype(jnp.bfloat16)

def apply_kernel(scaled, vector_half):
    total_rows = scaled.shape[1]
    block_rows = math.gcd(total_rows, 2048)
    blocked = scaled.reshape(scaled.shape[0], total_rows // block_rows, block_rows).transpose(1, 0, 2)
    products = lax.map(lambda block_points: jnp.dot(kernel_block(block_points, scaled), vector_half, preferred_element_type=jnp.float32), blocked)
    return products.reshape(total_rows, vector_half.shape[1])

def log_weight(alpha_list, beta_list):
    degree = len(alpha_list)
    width_probes = alpha_list[0].shape[0]
    zeros_row = jnp.zeros((width_probes,), jnp.float32)
    ones_row = jnp.ones((width_probes,), jnp.float32)
    matrix = []
    vectors = []
    for first_idx in range(degree):
        entries = []
        basis_row = []
        for second_idx in range(degree):
            if first_idx == second_idx:
                entries.append(alpha_list[first_idx])
                basis_row.append(ones_row)
            elif abs(first_idx - second_idx) == 1:
                entries.append(beta_list[min(first_idx, second_idx)])
                basis_row.append(zeros_row)
            else:
                entries.append(zeros_row)
                basis_row.append(zeros_row)
        matrix.append(entries)
        vectors.append(basis_row)
    for sweep_index in range(jacobi_sweeps):
        for first_idx in range(degree):
            for second_idx in range(first_idx + 1, degree):
                coupling = matrix[first_idx][second_idx]
                rotate_by = 0.5 * jnp.arctan2(2.0 * coupling, matrix[second_idx][second_idx] - matrix[first_idx][first_idx])
                cosine = jnp.cos(rotate_by)
                sine_val = jnp.sin(rotate_by)
                for row_idx in range(degree):
                    left_val = matrix[row_idx][first_idx]
                    right_val = matrix[row_idx][second_idx]
                    matrix[row_idx][first_idx] = cosine * left_val - sine_val * right_val
                    matrix[row_idx][second_idx] = sine_val * left_val + cosine * right_val
                    left_vec = vectors[row_idx][first_idx]
                    right_vec = vectors[row_idx][second_idx]
                    vectors[row_idx][first_idx] = cosine * left_vec - sine_val * right_vec
                    vectors[row_idx][second_idx] = sine_val * left_vec + cosine * right_vec
                for col_idx in range(degree):
                    upper_val = matrix[first_idx][col_idx]
                    lower_val = matrix[second_idx][col_idx]
                    matrix[first_idx][col_idx] = cosine * upper_val - sine_val * lower_val
                    matrix[second_idx][col_idx] = sine_val * upper_val + cosine * lower_val
    total = zeros_row
    for index_k in range(degree):
        total = total + vectors[0][index_k] * vectors[0][index_k] * jnp.log(matrix[index_k][index_k])
    return total

def reference(points, inverse_scales, probe_signs):
    scaled = points * inverse_scales[:, None]
    direction = 2.0 * probe_signs.astype(jnp.float32) - 1.0
    basis_prev = jnp.zeros_like(direction)
    alpha_list = []
    beta_list = []
    for lanczos_step in range(STEPS):
        squares = lax.optimization_barrier(jnp.sum(direction * direction, axis=0))
        image = apply_kernel(scaled, direction.astype(jnp.bfloat16)) + noise_level * direction
        curvature = lax.optimization_barrier(jnp.sum(direction * image, axis=0))
        beta_now = jnp.sqrt(squares + epsilon)
        alpha_now = curvature / (beta_now * beta_now)
        alpha_list.append(alpha_now)
        beta_list.append(beta_now)
        if lanczos_step + 1 < STEPS:
            basis_now = direction / beta_now
            direction = image / beta_now - alpha_now * basis_now - beta_now * basis_prev
            basis_prev = basis_now
    logdet_terms = log_weight(alpha_list, beta_list[1:])
    return (alpha_list[0], logdet_terms)
```

```python
import functools
import math

import jax
import jax.numpy as jnp
from jax import lax
from jax.experimental import pallas as pl
from jax.experimental.pallas import tpu as pltpu
from jax.sharding import PartitionSpec as P

STEPS = 3


epsilon = 1e-06
noise_level = 1.0
jacobi_sweeps = 6
MESH = pl.DeviceIdType.MESH


def flip(index, mask):
    bit = 1
    out = index
    while bit <= mask:
        if mask & bit:
            out = out + bit * (1 - 2 * ((index // bit) % 2))
        bit *= 2
    return out


def bits_below(count):
    return [1 << k for k in range(16) if (1 << k) < count]


def three_parts(x):
    high = x.astype(jnp.bfloat16).astype(jnp.float32)
    rest = x - high
    middle = rest.astype(jnp.bfloat16).astype(jnp.float32)
    low = (rest - middle).astype(jnp.bfloat16).astype(jnp.float32)
    return high, middle, low


def features(x, left):
    high, middle, low = three_parts(x)
    norm = -0.5 * jnp.sum(x * x, axis=0, keepdims=True)
    parts = three_parts(norm)
    rows = lax.broadcasted_iota(jnp.int32, x.shape, 0)
    first = 0 if left else 3
    ones_at = 3 if left else 0
    tail = jnp.where((rows >= ones_at) & (rows < ones_at + 3), 1.0, 0.0)
    for k in range(3):
        tail = jnp.where(rows == first + k, parts[k], tail)
    blank = jnp.zeros_like(x)
    if left:
        groups = [high, high, middle, middle, high, low, tail, blank]
    else:
        groups = [high, middle, high, middle, low, high, tail, blank]
    return jnp.concatenate(groups, axis=0)


def tree_sum(values):
    while len(values) > 1:
        values = [values[k] + values[k + 1] for k in range(0, len(values), 2)]
    return values[0]


def plain_sum(values):
    result = values[0]
    for value in values[1:]:
        result = result + value
    return result


def kernel(
    rows, cols,
    pts_ref, signs_ref,
    sums_ref, far_ref,
    near, stage, vecs, points, plane_points, left, right, total, direction, before,
    rs_out, rs_in, sums_out, sums_mid, sums_col, sums_row,
    pts_recv, pts_send, vec_recv, vec_send, ppts_recv, ppts_send,
    rs_recv, rs_send, write_sem, read_sem,
    col_recv, col_send, row_recv, row_send,
):
    slots, plane = 2 * rows, cols // 2
    n = pts_ref.shape[1]
    probes = signs_ref.shape[0]
    my_row, my_col = lax.axis_index("row"), lax.axis_index("col")
    tile = math.gcd(n, 256)
    half = n // 2

    def device(row_off, col_off):
        return (flip(my_row, row_off), flip(my_col, col_off))

    def remote(src, dst, send_sem, recv_sem, row_off, col_off):
        return pltpu.make_async_remote_copy(
            src_ref=src, dst_ref=dst, send_sem=send_sem, recv_sem=recv_sem,
            device_id=device(row_off, col_off), device_id_type=MESH,
        )

    def own_copies(buffer, own, recv, send):
        copies = [remote(own, buffer.at[1], send.at[rows], recv.at[1], 0, 1)]
        for off in range(1, rows):
            copies.append(remote(own, buffer.at[2 * off], send.at[off], recv.at[2 * off], off, 0))
        return copies

    def forward(buffer, recv, send, off):
        return remote(
            buffer.at[2 * off], buffer.at[2 * off + 1],
            send.at[rows + off], recv.at[2 * off + 1], 0, 1,
        )

    def poll(packs, slot):
        @pl.when(slot > 0)
        def _():
            for buffer, _, recv, send in packs:
                remote(buffer.at[slot], buffer.at[slot], send.at[0], recv.at[slot], 0, 1).wait_recv()

        @pl.when((slot > 0) & (slot % 2 == 0))
        def _():
            for buffer, _, recv, send in packs:
                forward(buffer, recv, send, slot // 2).start()

    def sent(buffer, own, recv, send):
        for copy in own_copies(buffer, own, recv, send):
            copy.wait_send()
        for off in range(1, rows):
            forward(buffer, recv, send, off).wait_send()

    def plane_copies(buffer, own, recv, send):
        return [
            remote(own, buffer.at[t], send.at[t], recv.at[t], 0, 2 * t) for t in range(1, plane)
        ]

    barrier = pltpu.get_barrier_semaphore()
    peers = [(0, c) for c in range(1, cols)] + [(r, 0) for r in range(1, rows)]
    for peer in peers:
        pl.semaphore_signal(barrier, inc=1, device_id=device(*peer), device_id_type=MESH)
    pl.semaphore_wait(barrier, len(peers))

    pts = (points, pts_ref, pts_recv, pts_send)
    plane_pts = plane_copies(plane_points, pts_ref, ppts_recv, ppts_send)
    for copy in plane_pts + own_copies(*pts):
        copy.start()
    pack = (vecs, signs_ref, vec_recv, vec_send)
    for copy in own_copies(*pack):
        copy.start()
    points[0] = pts_ref[...]
    vecs[0] = signs_ref[...]
    direction[...] = signs_ref[...].astype(jnp.float32)
    right[0] = features(pts_ref[...], False).astype(jnp.bfloat16)
    for t in range(1, plane):
        plane_pts[t - 1].wait_recv()
        right[t] = features(plane_points[t], False).astype(jnp.bfloat16)

    def write(slot, block):
        return pltpu.make_async_copy(stage.at[slot], far_ref.at[block], write_sem.at[slot])

    def read(slot, block):
        return pltpu.make_async_copy(far_ref.at[block], stage.at[slot], read_sem.at[slot])

    def column_sums(x):
        width = math.gcd(n, 128)
        folded = sum(x[:, s : s + width] for s in range(0, n, width))
        return jnp.sum(folded.T, axis=0, keepdims=True)

    def exchange(step, squares, curvature):
        sums_out[step] = jnp.concatenate(
            [squares, curvature, jnp.zeros((6, probes), jnp.float32)], axis=0
        )
        for source, target, recv, send, count, across in (
            (sums_out, sums_col, col_recv, col_send, cols, False),
            (sums_mid, sums_row, row_recv, row_send, rows, True),
        ):
            moves = [
                pltpu.make_async_remote_copy(
                    src_ref=source.at[step],
                    dst_ref=target.at[step, off],
                    send_sem=send.at[step, off],
                    recv_sem=recv.at[step, off],
                    device_id=device(off, 0) if across else device(0, off),
                    device_id_type=MESH,
                )
                for off in range(1, count)
            ]
            for move in moves:
                move.start()
            for move in moves:
                move.wait()
            result = tree_sum(
                [source[step]] + [target[step, off] for off in range(1, count)]
            )
            if not across:
                sums_mid[step] = result
        return result

    def spread(row):
        return jnp.broadcast_to(row, (probes, probes)).T

    def reduce_image():
        bits = bits_below(plane)
        number, count = {}, 0
        for s in range(len(bits)):
            for u in range(plane >> (s + 1)):
                number[(s, u)] = count
                count += 1
        orders = [bits, bits[::-1]]

        def spots(order, s):
            done = sum(order[: s + 1])
            return [u for u in range(plane) if not u & done]

        def copy(h, s, k):
            i = number[(s, k)]
            return remote(
                rs_out.at[h, i], rs_in.at[h, i], rs_send.at[h, i], rs_recv.at[h, i],
                0, 2 * orders[h][s],
            )

        def received(h, s, t):
            k = spots(orders[h], s).index(t)
            copy(h, s, k).wait_recv()
            return rs_in[h, number[(s, k)]].astype(jnp.float32)

        for s in range(len(bits)):
            for back in range(plane >> (s + 1)):
                for h in range(2):
                    u = spots(orders[h], s)
                    k = len(u) - 1 - back
                    t = u[k] | orders[h][s]
                    part = total[t, :, h * half : (h + 1) * half]
                    for earlier in range(s):
                        part = part + received(h, earlier, t)
                    rs_out[h, number[(s, k)]] = part.astype(jnp.bfloat16)
                    copy(h, s, k).start()
        for h in range(2):
            span = slice(h * half, (h + 1) * half)
            total[0, :, span] += plain_sum([received(h, s, 0) for s in range(len(bits))])
        for h in range(2):
            for s in range(len(bits)):
                for k in range(plane >> (s + 1)):
                    copy(h, s, k).wait_send()

    for step in range(STEPS):
        for t in range(plane):
            total[t] = jnp.zeros((probes, n), jnp.float32)
        if step > 0:
            pack = (vecs, vecs.at[0], vec_recv, vec_send)
            for copy in own_copies(*pack):
                copy.start()
        if step + 1 == STEPS:
            plane_vec = [
                remote(
                    vecs.at[0, :, h * half : (h + 1) * half], rs_in.at[h, t - 1],
                    rs_send.at[h, t - 1], rs_recv.at[h, t - 1], 0, 2 * t,
                )
                for t in range(1, plane) for h in range(2)
            ]
            for copy in plane_vec:
                copy.start()
        if step == 0:
            def first(c, carry):
                poll((pts, pack), c)
                slot = lax.rem(c, 2)

                @pl.when(c >= 2)
                def _():
                    write(slot, c - 2).wait()

                left[...] = features(points[c], True).T.astype(jnp.bfloat16)

                def chunk(t):
                    return stage.at[slot] if t == plane - 1 else near.at[c, t]

                for t in range(plane + 1):
                    parts = []
                    for s in range(0, n, tile):
                        part = slice(s, s + tile)
                        if t < plane:
                            power = jnp.dot(
                                left[part, :], right[t], preferred_element_type=jnp.float32
                            )
                            chunk(t)[part, :] = jnp.exp2(jnp.minimum(power, 0.0)).astype(jnp.bfloat16)
                        if t > 0:
                            parts.append(jnp.dot(
                                vecs[c, :, part], chunk(t - 1)[part, :],
                                preferred_element_type=jnp.float32,
                            ))
                    if t == plane - 1:
                        write(slot, c).start()
                    if t > 0:
                        total[t - 1] += sum(parts[1:], parts[0])
                return carry

            lax.fori_loop(0, slots, first, 0)
            for c in range(max(slots - 2, 0), slots):
                write(c % 2, c).wait()
        else:
            def later(c, carry):
                poll((pack,), c)
                slot = lax.rem(c, 2)

                @pl.when(c + 1 < slots)
                def _():
                    read(1 - slot, c + 1).start()

                for t in range(plane - 1):
                    total[t] += jnp.dot(
                        vecs[c], near[c, t], preferred_element_type=jnp.float32
                    )
                read(slot, c).wait()
                total[plane - 1] += jnp.dot(
                    vecs[c], stage[slot], preferred_element_type=jnp.float32
                )
                return carry

            read(0, 0).start()
            lax.fori_loop(0, slots, later, 0)
        sent(*pack)
        if step == 0:
            sent(*pts)
            for copy in plane_pts:
                copy.wait_send()
        now = direction[...]
        if step + 1 < STEPS:
            reduce_image()
            image = total[0] + noise_level * now
            curvature = column_sums(now * image)
        else:
            for copy in plane_vec:
                copy.wait()
            for h in range(2):
                span = slice(h * half, (h + 1) * half)
                product = now[:, span] * (total[0, :, span] + noise_level * now[:, span])
                for t in range(1, plane):
                    product = product + rs_in[h, t - 1].astype(jnp.float32) * total[t, :, span]
                before[:, span] = product
            curvature = column_sums(before[...])
        result = exchange(step, column_sums(now * now), curvature)
        squares, curvature = result[0:1], result[1:2]
        sums_ref[step] = result
        if step + 1 < STEPS:
            beta = jnp.sqrt(squares + epsilon)
            alpha = curvature / (beta * beta)
            inverse = spread(1.0 / beta)
            alpha_all, beta_all = spread(alpha), spread(beta)
            for s in range(0, n, 128):
                part = slice(s, s + 128)
                basis = direction[:, part] * inverse
                fresh = (total[0, :, part] + noise_level * direction[:, part]) * inverse - alpha_all * basis
                if step > 0:
                    fresh = fresh - beta_all * before[:, part]
                before[:, part] = basis
                direction[:, part] = fresh
                vecs[0, :, part] = fresh.astype(jnp.bfloat16)


def log_weight(alpha_list, beta_list):
    degree = len(alpha_list)
    width_probes = alpha_list[0].shape[0]
    zeros_row = jnp.zeros((width_probes,), jnp.float32)
    ones_row = jnp.ones((width_probes,), jnp.float32)
    matrix = []
    vectors = []
    for first_idx in range(degree):
        entries = []
        basis_row = []
        for second_idx in range(degree):
            if first_idx == second_idx:
                entries.append(alpha_list[first_idx])
                basis_row.append(ones_row)
            elif abs(first_idx - second_idx) == 1:
                entries.append(beta_list[min(first_idx, second_idx)])
                basis_row.append(zeros_row)
            else:
                entries.append(zeros_row)
                basis_row.append(zeros_row)
        matrix.append(entries)
        vectors.append(basis_row)
    for sweep_index in range(jacobi_sweeps):
        for first_idx in range(degree):
            for second_idx in range(first_idx + 1, degree):
                coupling = matrix[first_idx][second_idx]
                rotate_by = 0.5 * jnp.arctan2(
                    2.0 * coupling, matrix[second_idx][second_idx] - matrix[first_idx][first_idx]
                )
                cosine = jnp.cos(rotate_by)
                sine_val = jnp.sin(rotate_by)
                for row_idx in range(degree):
                    left_val = matrix[row_idx][first_idx]
                    right_val = matrix[row_idx][second_idx]
                    matrix[row_idx][first_idx] = cosine * left_val - sine_val * right_val
                    matrix[row_idx][second_idx] = sine_val * left_val + cosine * right_val
                    left_vec = vectors[row_idx][first_idx]
                    right_vec = vectors[row_idx][second_idx]
                    vectors[row_idx][first_idx] = cosine * left_vec - sine_val * right_vec
                    vectors[row_idx][second_idx] = sine_val * left_vec + cosine * right_vec
                for col_idx in range(degree):
                    upper_val = matrix[first_idx][col_idx]
                    lower_val = matrix[second_idx][col_idx]
                    matrix[first_idx][col_idx] = cosine * upper_val - sine_val * lower_val
                    matrix[second_idx][col_idx] = sine_val * upper_val + cosine * lower_val
    total = zeros_row
    for index_k in range(degree):
        total = total + vectors[0][index_k] * vectors[0][index_k] * jnp.log(
            matrix[index_k][index_k]
        )
    return total


def per_device(rows, cols, points, inverse_scales, probe_signs):
    dims, n = points.shape
    probes = probe_signs.shape[1]
    slots, plane = 2 * rows, cols // 2
    scaled = points * inverse_scales[:, None] * math.sqrt(math.log2(math.e))
    signs = (2.0 * probe_signs.astype(jnp.float32) - 1.0).T.astype(jnp.bfloat16)
    dma = pltpu.SemaphoreType.DMA
    vmem = pltpu.VMEM
    sums, _ = pl.pallas_call(
        functools.partial(kernel, rows, cols),
        out_shape=(
            jax.ShapeDtypeStruct((STEPS, 8, probes), jnp.float32),
            jax.ShapeDtypeStruct((slots, n, n), jnp.bfloat16),
        ),
        in_specs=[pl.BlockSpec(memory_space=pltpu.VMEM)] * 2,
        out_specs=(
            pl.BlockSpec(memory_space=pltpu.VMEM),
            pl.BlockSpec(memory_space=pl.ANY),
        ),
        scratch_shapes=[
            vmem((slots, plane - 1, n, n), jnp.bfloat16),
            vmem((2, n, n), jnp.bfloat16),
            vmem((slots, probes, n), jnp.bfloat16),
            vmem((slots, dims, n), jnp.float32),
            vmem((plane, dims, n), jnp.float32),
            vmem((n, 8 * dims), jnp.bfloat16),
            vmem((plane, 8 * dims, n), jnp.bfloat16),
            vmem((plane, probes, n), jnp.float32),
            vmem((probes, n), jnp.float32),
            vmem((probes, n), jnp.float32),
            vmem((2, plane - 1, probes, n // 2), jnp.bfloat16),
            vmem((2, plane - 1, probes, n // 2), jnp.bfloat16),
            vmem((STEPS, 8, probes), jnp.float32),
            vmem((STEPS, 8, probes), jnp.float32),
            vmem((STEPS, cols, 8, probes), jnp.float32),
            vmem((STEPS, rows, 8, probes), jnp.float32),
            dma((slots,)),
            dma((slots,)),
            dma((slots,)),
            dma((slots,)),
            dma((plane,)),
            dma((plane,)),
            dma((2, plane - 1)),
            dma((2, plane - 1)),
            dma((2,)),
            dma((2,)),
            dma((STEPS, cols)),
            dma((STEPS, cols)),
            dma((STEPS, rows)),
            dma((STEPS, rows)),
        ],
        compiler_params=pltpu.CompilerParams(
            collective_id=0, has_side_effects=True, vmem_limit_bytes=64 * 2**20 - 65536
        ),
        name="lanczos",
    )(scaled, signs)
    beta_list = [jnp.sqrt(sums[k, 0] + epsilon) for k in range(STEPS)]
    alpha_list = [sums[k, 1] / (beta_list[k] * beta_list[k]) for k in range(STEPS)]
    return alpha_list[0], log_weight(alpha_list, beta_list[1:])


def solution(mesh):
    in_specs = (P(None, ("row", "col")), P(), P(("row", "col"), None))
    out_specs = (P(), P())
    return jax.shard_map(
        functools.partial(per_device, mesh.shape["row"], mesh.shape["col"]),
        mesh=mesh, in_specs=in_specs, out_specs=out_specs, check_vma=False,
    )
```

```python
import functools
import math

import jax
import jax.numpy as jnp
from jax import lax
from jax.experimental import pallas as pl
from jax.experimental.pallas import tpu as pltpu
from jax.sharding import PartitionSpec as P

STEPS = 3


epsilon = 1e-06
noise_level = 1.0
jacobi_sweeps = 6
MESH = pl.DeviceIdType.MESH


def flip(index, mask):
    bit = 1
    out = index
    while bit <= mask:
        if mask & bit:
            out = out + bit * (1 - 2 * ((index // bit) % 2))
        bit *= 2
    return out


def bits_below(count):
    return [1 << k for k in range(16) if (1 << k) < count]


def three_parts(x):
    high = x.astype(jnp.bfloat16).astype(jnp.float32)
    rest = x - high
    middle = rest.astype(jnp.bfloat16).astype(jnp.float32)
    low = (rest - middle).astype(jnp.bfloat16).astype(jnp.float32)
    return high, middle, low


def features(x, left):
    high, middle, low = three_parts(x)
    norm = -0.5 * jnp.sum(x * x, axis=0, keepdims=True)
    parts = three_parts(norm)
    rows = lax.broadcasted_iota(jnp.int32, x.shape, 0)
    first = 0 if left else 3
    ones_at = 3 if left else 0
    tail = jnp.where((rows >= ones_at) & (rows < ones_at + 3), 1.0, 0.0)
    for k in range(3):
        tail = jnp.where(rows == first + k, parts[k], tail)
    blank = jnp.zeros_like(x)
    if left:
        groups = [high, high, middle, middle, high, low, tail, blank]
    else:
        groups = [high, middle, high, middle, low, high, tail, blank]
    return jnp.concatenate(groups, axis=0)


def tree_sum(values):
    while len(values) > 1:
        values = [values[k] + values[k + 1] for k in range(0, len(values), 2)]
    return values[0]


def plain_sum(values):
    result = values[0]
    for value in values[1:]:
        result = result + value
    return result


def kernel(
    rows, cols,
    pts_ref, scale_ref, signs_ref,
    sums_ref, far_ref,
    near, stage, vecs, points, plane_points, plane_vecs, left, right, total, start, image,
    rs_out, rs_in, sums_out, sums_in,
    pts_recv, pts_send, vec_recv, vec_send, ppts_recv, ppts_send, pvec_recv, pvec_send,
    rs_recv, rs_send, write_sem, read_sem, sum_recv, sum_send, free_sem,
):
    slots, plane, devices = 2 * rows, cols // 2, rows * cols
    n, probes = pts_ref.shape[1], signs_ref.shape[1]
    my_row, my_col = lax.axis_index("row"), lax.axis_index("col")
    half = n // 2
    tile = math.gcd(half, 256)
    halves = [slice(h * half, (h + 1) * half) for h in range(2)]
    bits = bits_below(plane)

    def device(row_off, col_off):
        return (flip(my_row, row_off), flip(my_col, col_off))

    def remote(src, dst, send_sem, recv_sem, row_off, col_off):
        return pltpu.make_async_remote_copy(
            src_ref=src, dst_ref=dst, send_sem=send_sem, recv_sem=recv_sem,
            device_id=device(row_off, col_off), device_id_type=MESH,
        )

    def own_copy(pack, part, off):
        buffer, recv, send = pack
        slot = 2 * off if off else 1
        return remote(
            buffer.at[part, 0], buffer.at[part, slot], send.at[part, off], recv.at[part, slot],
            off, 0 if off else 1,
        )

    def forward(pack, part, off):
        buffer, recv, send = pack
        return remote(
            buffer.at[part, 2 * off], buffer.at[part, 2 * off + 1],
            send.at[part, rows + off], recv.at[part, 2 * off + 1], 0, 1,
        )

    def poll(pack, part, slot):
        buffer, recv, send = pack

        @pl.when(slot > 0)
        def _():
            remote(
                buffer.at[part, slot], buffer.at[part, slot], send.at[0, 0], recv.at[part, slot], 0, 1
            ).wait_recv()

        @pl.when((slot > 0) & (slot % 2 == 0))
        def _():
            forward(pack, part, slot // 2).start()

    def sent(pack, part):
        for off in range(rows):
            own_copy(pack, part, off).wait_send()
        for off in range(1, rows):
            forward(pack, part, off).wait_send()

    def plane_copy(part, t):
        return remote(
            vecs.at[part, 0], plane_vecs.at[part, t - 1],
            pvec_send.at[part, t - 1], pvec_recv.at[part, t - 1], 0, 2 * t,
        )

    def column_sums(x):
        width = math.gcd(n, 128)
        folded = sum(x[:, s : s + width] for s in range(0, x.shape[1], width))
        return jnp.sum(folded.T, axis=0, keepdims=True)

    def spread(row):
        return jnp.broadcast_to(row, (probes, probes)).T

    def wide(row, width):
        return jnp.concatenate([spread(row)] * (width // probes), axis=1)

    def sum_copy(step, off):
        return remote(
            sums_out.at[step], sums_in.at[step, off], sum_send.at[step, off], sum_recv.at[step, off],
            off // cols, off % cols,
        )

    def give(step, squares, curvature):
        sums_out[step] = jnp.concatenate(
            [squares, curvature, jnp.zeros((6, probes), jnp.float32)], axis=0
        )
        for off in range(1, devices):
            sum_copy(step, off).start()

    def take(step):
        for off in range(1, devices):
            sum_copy(step, off).wait()
        result = tree_sum([sums_out[step]] + [sums_in[step, off] for off in range(1, devices)])
        sums_ref[step] = result
        squares, curvature = result[0:1], result[1:2]
        beta = jnp.sqrt(squares + epsilon)
        return curvature / (beta * beta), beta

    number, count = {}, 0
    for s in range(len(bits)):
        for u in range(plane >> (s + 1)):
            number[(s, u)] = count
            count += 1
    orders = [bits, bits[::-1]]

    def spots(h, s):
        done = sum(orders[h][: s + 1])
        return [u for u in range(plane) if not u & done]

    def reduce_copy(h, s, k):
        i = number[(s, k)]
        return remote(
            rs_out.at[h, i], rs_in.at[h, i], rs_send.at[h, i], rs_recv.at[h, i],
            0, 2 * orders[h][s],
        )

    def received(h, s, t):
        k = spots(h, s).index(t)
        reduce_copy(h, s, k).wait_recv()
        return rs_in[h, number[(s, k)]].astype(jnp.float32)

    def reduce_stage(h, s, k):
        t = spots(h, s)[k] | orders[h][s]
        part = total[t, :, halves[h]]
        for earlier in range(s):
            part = part + received(h, earlier, t)
        rs_out[h, number[(s, k)]] = part.astype(jnp.bfloat16)
        reduce_copy(h, s, k).start()

    def reduce_rest(h):
        for s in range(1, len(bits)):
            for k in reversed(range(plane >> (s + 1))):
                reduce_stage(h, s, k)

    def reduced(h):
        value = total[0, :, halves[h]]
        for s in range(len(bits)):
            value = value + received(h, s, 0)
        return value

    def reduce_sent():
        for h in range(2):
            for s in range(len(bits)):
                for k in range(plane >> (s + 1)):
                    reduce_copy(h, s, k).wait_send()

    vec_pack = (vecs, vec_recv, vec_send)
    pts_pack = (points, pts_recv, pts_send)

    def send_own(h):
        for off in range(1, rows):
            own_copy(vec_pack, h, off).start()
        own_copy(vec_pack, h, 0).start()
        for t in range(1, plane):
            plane_copy(h, t).start()

    barrier = pltpu.get_barrier_semaphore()
    peers = [(r, c) for r in range(rows) for c in range(cols) if r or c]
    for peer in peers:
        pl.semaphore_signal(barrier, inc=1, device_id=device(*peer), device_id_type=MESH)

    dims = pts_ref.shape[0]
    index = lax.broadcasted_iota(jnp.int32, (dims, n), 0)
    scale = jnp.zeros((dims, n), jnp.float32)
    for d in range(dims):
        scale = jnp.where(index == d, scale_ref[d], scale)
    points[0, 0] = pts_ref[...] * scale * math.sqrt(math.log2(math.e))
    for s in range(0, n, 128):
        width = min(128, n)
        flipped = (2.0 * signs_ref[s : s + width, :].astype(jnp.float32) - 1.0).T
        start[:, s : s + width] = flipped.astype(jnp.bfloat16)
        vecs[s // half, 0, :, s % half : s % half + width] = flipped.astype(jnp.bfloat16)
    pl.semaphore_wait(barrier, len(peers))

    def plane_point_copy(t):
        return remote(
            points.at[0, 0], plane_points.at[t - 1], ppts_send.at[t - 1], ppts_recv.at[t - 1], 0, 2 * t
        )

    for t in range(1, plane):
        plane_point_copy(t).start()
    for off in range(1, rows):
        own_copy(pts_pack, 0, off).start()
    own_copy(pts_pack, 0, 0).start()
    for off in range(rows):
        for h in range(2):
            own_copy(vec_pack, h, off).start()
    right[0] = features(points[0, 0], False).astype(jnp.bfloat16)
    for t in range(plane):
        total[t] = jnp.zeros((probes, n), jnp.float32)
    for t in range(1, plane):
        plane_point_copy(t).wait()
        right[t] = features(plane_points[t - 1], False).astype(jnp.bfloat16)

    def write(slot, h, c):
        return pltpu.make_async_copy(
            stage.at[2 * slot + h], far_ref.at[c, pl.ds(h * half, half)], write_sem.at[slot, h]
        )

    def read(slot, h, c):
        return pltpu.make_async_copy(
            far_ref.at[c, pl.ds(pl.multiple_of(h * half, half), half)], stage.at[slot], read_sem.at[slot]
        )

    def block(c, t, s, cut=slice(None)):
        if t == plane - 1:
            return stage.at[2 * lax.rem(c, 2) + s // half, s % half : s % half + tile, cut]
        return near.at[c, t, s : s + tile, cut]

    def vec(c, s):
        return vecs[s // half, c, :, s % half : s % half + tile]

    def first(c, forming, applying):
        slot = lax.rem(c, 2)
        order = [plane - 1] + list(range(plane - 1))
        if forming:
            poll(pts_pack, 0, c)
            left[...] = features(points[0, c], True).T.astype(jnp.bfloat16)
        if applying:
            for h in range(2):
                poll(vec_pack, h, c - 2)
                write(slot, h, c - 2).wait()
        for t in range(plane):
            parts = []
            for s in range(0, n, tile):
                if forming:
                    power = jnp.dot(
                        left[s : s + tile, :], right[t], preferred_element_type=jnp.float32
                    )
                    block(c, t, s)[...] = jnp.exp2(jnp.minimum(power, 0.0)).astype(jnp.bfloat16)
                if applying:
                    parts.append(jnp.dot(
                        vec(c - 2, s), block(c - 2, order[t], s)[...],
                        preferred_element_type=jnp.float32,
                    ))
            if applying:
                total[order[t]] += plain_sum(parts)
        if forming:
            for h in range(2):
                write(slot, h, c).start()

    def loop(low, high, forming, applying):
        def body(c, carry):
            first(c, forming, applying)
            return carry

        lax.fori_loop(low, high, body, 0)

    loop(0, 2, True, False)
    loop(2, slots, True, True)
    last = [slots - 2, slots - 1]
    for c in last:
        for h in range(2):
            poll(vec_pack, h, c)
    for h in range(2):
        for t in reversed(range(plane)):
            parts = [
                jnp.dot(vec(c, s), block(c, t, s, halves[h])[...], preferred_element_type=jnp.float32)
                for c in last for s in range(0, n, tile)
            ]
            total[t, :, halves[h]] += plain_sum(parts)
            for k, u in enumerate(spots(h, 0)):
                if u | orders[h][0] == t:
                    reduce_stage(h, 0, k)
    for c in last:
        for h in range(2):
            write(c % 2, h, c).wait()
    for h in range(2):
        sent(vec_pack, h)
    sent(pts_pack, 0)
    for off in range(rows):
        pl.semaphore_signal(
            free_sem, inc=1, device_id=device(off, 0 if off else 1), device_id_type=MESH
        )

    ring = 4
    for i in range(min(ring - 1, 2 * slots)):
        read(i, i // slots, i % slots).start()

    both, cross, own = [], [], []
    for h in range(2):
        reduce_rest(h)
        value = reduced(h)
        now = start[:, halves[h]].astype(jnp.float32)
        image[:, halves[h]] = value
        vecs[h, 0] = (value - now).astype(jnp.bfloat16)
        if h == 0:
            pl.semaphore_wait(free_sem, rows)
        send_own(h)
        both.append(column_sums(now * value))
        cross.append(column_sums(value * (value - now)))
        own.append(column_sums(now * now))
    reduce_sent()
    both, cross, own = both[0] + both[1], cross[0] + cross[1], own[0] + own[1]
    give(0, own, both + noise_level * own)

    def product():
        def later(i, carry):
            h, c = i // slots, lax.rem(i, slots)
            poll(vec_pack, h, c)
            slot = lax.rem(i, ring)

            @pl.when(i + ring - 1 < 2 * slots)
            def _():
                ahead = i + ring - 1
                read(lax.rem(ahead, ring), ahead // slots, lax.rem(ahead, slots)).start()

            for t in range(plane):
                if t == plane - 1:
                    read(slot, h, c).wait()
                    matrix = stage[slot]
                else:
                    matrix = near[c, t, pl.ds(pl.multiple_of(h * half, half), half), :]
                total[t] += jnp.dot(vecs[h, c], matrix, preferred_element_type=jnp.float32)
            return carry

        for t in range(plane):
            total[t] = jnp.zeros((probes, n), jnp.float32)
        lax.fori_loop(0, 2 * slots, later, 0)
        for h in range(2):
            sent(vec_pack, h)

    def plane_arrived():
        for h in range(2):
            for t in range(1, plane):
                plane_copy(h, t).wait()

    def plane_products(h):
        value = 0.0
        for t in range(1, plane):
            value = value + plane_vecs[h, t - 1].astype(jnp.float32) * total[t, :, halves[h]]
        return value

    product()
    plane_arrived()
    for k in reversed(range(plane // 2)):
        for h in range(2):
            reduce_stage(h, 0, k)
    for i in range(min(ring - 1, 2 * slots)):
        read(i, i // slots, i % slots).start()
    alpha_1, beta_1 = take(0)
    shift = (1.0 + noise_level) - alpha_1
    inverse_1 = 1.0 / beta_1
    shift_half, inverse_half = wide(shift, half), wide(inverse_1, half)
    square, form = 0.0, 0.0
    for h in range(2):
        span = halves[h]
        now = start[:, span].astype(jnp.float32)
        excess = image[:, span] - now
        fresh = (excess + shift_half * now) * inverse_half
        square = square + column_sums(fresh * fresh)
        form = form + column_sums(excess * total[0, :, span] + plane_products(h))
    form = (form + 2.0 * shift * cross + shift * shift * both) * inverse_1 * inverse_1
    give(1, square, form + noise_level * square)
    for h in range(2):
        reduce_rest(h)
    alpha_2, beta_2 = take(1)
    inverse_2 = 1.0 / beta_2
    scale_now = wide(inverse_2 * inverse_1, half)
    minus, back = wide(alpha_2 * inverse_2, half), wide(beta_2 * inverse_1, half)
    square = 0.0
    for h in range(2):
        span = halves[h]
        now, old = start[:, span].astype(jnp.float32), image[:, span]
        value = (reduced(h) + shift_half * old) * scale_now
        direction = (old - now + shift_half * now) * inverse_half
        value = value + (noise_level * wide(inverse_2, half) - minus) * direction - back * now
        vecs[h, 0] = value.astype(jnp.bfloat16)
        send_own(h)
        image[:, span] = value
        square = square + column_sums(value * value)
    reduce_sent()

    product()
    plane_arrived()
    form = 0.0
    for h in range(2):
        span = halves[h]
        form = form + column_sums(image[:, span] * total[0, :, span] + plane_products(h))
    give(2, square, form + noise_level * square)
    take(2)


def log_weight(alpha_list, beta_list):
    degree = len(alpha_list)
    width_probes = alpha_list[0].shape[0]
    zeros_row = jnp.zeros((width_probes,), jnp.float32)
    ones_row = jnp.ones((width_probes,), jnp.float32)
    matrix = []
    vectors = []
    for first_idx in range(degree):
        entries = []
        basis_row = []
        for second_idx in range(degree):
            if first_idx == second_idx:
                entries.append(alpha_list[first_idx])
                basis_row.append(ones_row)
            elif abs(first_idx - second_idx) == 1:
                entries.append(beta_list[min(first_idx, second_idx)])
                basis_row.append(zeros_row)
            else:
                entries.append(zeros_row)
                basis_row.append(zeros_row)
        matrix.append(entries)
        vectors.append(basis_row)
    for sweep_index in range(jacobi_sweeps):
        for first_idx in range(degree):
            for second_idx in range(first_idx + 1, degree):
                coupling = matrix[first_idx][second_idx]
                rotate_by = 0.5 * jnp.arctan2(
                    2.0 * coupling, matrix[second_idx][second_idx] - matrix[first_idx][first_idx]
                )
                cosine = jnp.cos(rotate_by)
                sine_val = jnp.sin(rotate_by)
                for row_idx in range(degree):
                    left_val = matrix[row_idx][first_idx]
                    right_val = matrix[row_idx][second_idx]
                    matrix[row_idx][first_idx] = cosine * left_val - sine_val * right_val
                    matrix[row_idx][second_idx] = sine_val * left_val + cosine * right_val
                    left_vec = vectors[row_idx][first_idx]
                    right_vec = vectors[row_idx][second_idx]
                    vectors[row_idx][first_idx] = cosine * left_vec - sine_val * right_vec
                    vectors[row_idx][second_idx] = sine_val * left_vec + cosine * right_vec
                for col_idx in range(degree):
                    upper_val = matrix[first_idx][col_idx]
                    lower_val = matrix[second_idx][col_idx]
                    matrix[first_idx][col_idx] = cosine * upper_val - sine_val * lower_val
                    matrix[second_idx][col_idx] = sine_val * upper_val + cosine * lower_val
    total = zeros_row
    for index_k in range(degree):
        total = total + vectors[0][index_k] * vectors[0][index_k] * jnp.log(
            matrix[index_k][index_k]
        )
    return total


def per_device(rows, cols, points, inverse_scales, probe_signs):
    dims, n = points.shape
    probes = probe_signs.shape[1]
    slots, plane, devices = 2 * rows, cols // 2, rows * cols
    dma = pltpu.SemaphoreType.DMA
    vmem = pltpu.VMEM
    sums, _ = pl.pallas_call(
        functools.partial(kernel, rows, cols),
        out_shape=(
            jax.ShapeDtypeStruct((STEPS, 8, probes), jnp.float32),
            jax.ShapeDtypeStruct((slots, n, n), jnp.bfloat16),
        ),
        in_specs=[
            pl.BlockSpec(memory_space=pltpu.VMEM),
            pl.BlockSpec(memory_space=pltpu.SMEM),
            pl.BlockSpec(memory_space=pltpu.VMEM),
        ],
        out_specs=(
            pl.BlockSpec(memory_space=pltpu.VMEM),
            pl.BlockSpec(memory_space=pl.ANY),
        ),
        scratch_shapes=[
            vmem((slots, plane - 1, n, n), jnp.bfloat16),
            vmem((4, n // 2, n), jnp.bfloat16),
            vmem((2, slots, probes, n // 2), jnp.bfloat16),
            vmem((1, slots, dims, n), jnp.float32),
            vmem((plane - 1, dims, n), jnp.float32),
            vmem((2, plane - 1, probes, n // 2), jnp.bfloat16),
            vmem((n, 8 * dims), jnp.bfloat16),
            vmem((plane, 8 * dims, n), jnp.bfloat16),
            vmem((plane, probes, n), jnp.float32),
            vmem((probes, n), jnp.bfloat16),
            vmem((probes, n), jnp.float32),
            vmem((2, plane - 1, probes, n // 2), jnp.bfloat16),
            vmem((2, plane - 1, probes, n // 2), jnp.bfloat16),
            vmem((STEPS, 8, probes), jnp.float32),
            vmem((STEPS, devices, 8, probes), jnp.float32),
            dma((1, slots)),
            dma((1, slots)),
            dma((2, slots)),
            dma((2, slots)),
            dma((plane - 1,)),
            dma((plane - 1,)),
            dma((2, plane - 1)),
            dma((2, plane - 1)),
            dma((2, plane - 1)),
            dma((2, plane - 1)),
            dma((2, 2)),
            dma((4,)),
            dma((STEPS, devices)),
            dma((STEPS, devices)),
            pltpu.SemaphoreType.REGULAR,
        ],
        compiler_params=pltpu.CompilerParams(
            collective_id=0, has_side_effects=True, vmem_limit_bytes=64 * 2**20 - 65536
        ),
        name="lanczos",
    )(points, inverse_scales, probe_signs)
    beta_list = [jnp.sqrt(sums[k, 0] + epsilon) for k in range(STEPS)]
    alpha_list = [sums[k, 1] / (beta_list[k] * beta_list[k]) for k in range(STEPS)]
    return alpha_list[0], log_weight(alpha_list, beta_list[1:])


def solution(mesh):
    in_specs = (P(None, ("row", "col")), P(), P(("row", "col"), None))
    out_specs = (P(), P())
    return jax.shard_map(
        functools.partial(per_device, mesh.shape["row"], mesh.shape["col"]),
        mesh=mesh, in_specs=in_specs, out_specs=out_specs, check_vma=False,
    )
```

```python
import functools
import math

import jax
import jax.numpy as jnp
from jax import lax
from jax.experimental import pallas as pl
from jax.experimental.pallas import tpu as pltpu
from jax.sharding import PartitionSpec as P

STEPS = 3


epsilon = 1e-06
noise_level = 1.0
jacobi_sweeps = 6
MESH = pl.DeviceIdType.MESH


def flip(index, mask):
    bit = 1
    out = index
    while bit <= mask:
        if mask & bit:
            out = out + bit * (1 - 2 * ((index // bit) % 2))
        bit *= 2
    return out


def bits_below(count):
    return [1 << k for k in range(16) if (1 << k) < count]


def three_parts(x):
    high = x.astype(jnp.bfloat16).astype(jnp.float32)
    rest = x - high
    middle = rest.astype(jnp.bfloat16).astype(jnp.float32)
    low = (rest - middle).astype(jnp.bfloat16).astype(jnp.float32)
    return high, middle, low


def features(x, left):
    high, middle, low = three_parts(x)
    norm = -0.5 * jnp.sum(x * x, axis=0, keepdims=True)
    parts = three_parts(norm)
    rows = lax.broadcasted_iota(jnp.int32, x.shape, 0)
    first = 0 if left else 3
    ones_at = 3 if left else 0
    tail = jnp.where((rows >= ones_at) & (rows < ones_at + 3), 1.0, 0.0)
    for k in range(3):
        tail = jnp.where(rows == first + k, parts[k], tail)
    blank = jnp.zeros_like(x)
    if left:
        groups = [high, high, middle, middle, high, low, tail, blank]
    else:
        groups = [high, middle, high, middle, low, high, tail, blank]
    return jnp.concatenate(groups, axis=0)


def tree_sum(values):
    while len(values) > 1:
        values = [values[k] + values[k + 1] for k in range(0, len(values), 2)]
    return values[0]


def plain_sum(values):
    result = values[0]
    for value in values[1:]:
        result = result + value
    return result


def groups(rows, cols):
    gather = [(0, 1 << k) for k in range(1, 16, 2) if (1 << k) < cols]
    gather += [(1 << k, 0) for k in range(1, 16, 2) if (1 << k) < rows]
    other = [(0, 1 << k) for k in range(2, 16, 2) if (1 << k) < cols]
    other += [(1 << k, 0) for k in range(0, 16, 2) if (1 << k) < rows]

    def offsets(bits):
        table = [(0, 0)]
        for row_off, col_off in bits:
            table += [(r + row_off, c + col_off) for r, c in table]
        return table

    return offsets(gather), offsets(other)


def kernel(
    rows, cols,
    pts_ref, scale_ref, signs_ref,
    sums_ref, far_ref,
    near, stage, vecs, points, plane_points, plane_vecs, left, right, total, start, image,
    rs_out, rs_in, sums_out, sums_in,
    pts_recv, pts_send, vec_recv, vec_send, ppts_recv, ppts_send, pvec_recv, pvec_send,
    rs_recv, rs_send, write_sem, read_sem, sum_recv, sum_send, free_sem,
):
    gather, spread_over = groups(rows, cols)
    slots, plane, devices = 2 * len(gather), len(spread_over), rows * cols
    n, probes = pts_ref.shape[1], signs_ref.shape[1]
    my_row, my_col = lax.axis_index("row"), lax.axis_index("col")
    half = n // 2
    tile = math.gcd(half, 256)
    halves = [slice(h * half, (h + 1) * half) for h in range(2)]
    bits = bits_below(plane)

    def device(row_off, col_off):
        return (flip(my_row, row_off), flip(my_col, col_off))

    def remote(src, dst, send_sem, recv_sem, row_off, col_off):
        return pltpu.make_async_remote_copy(
            src_ref=src, dst_ref=dst, send_sem=send_sem, recv_sem=recv_sem,
            device_id=device(row_off, col_off), device_id_type=MESH,
        )

    chips = slots // 2
    singles = bits_below(chips)

    def own_copy(pack, part, chip):
        buffer, recv, send = pack
        slot = 2 * chip if chip else 1
        row_off, col_off = gather[chip] if chip else (0, 1)
        return remote(
            buffer.at[part, 0], buffer.at[part, slot], send.at[part, chip], recv.at[part, slot],
            row_off, col_off,
        )

    def forwards(pack, part, chip):
        buffer, recv, send = pack
        low = chip & -chip
        moves = [(2 * (chip | bit), gather[bit]) for bit in singles if bit < low]
        moves.append((2 * chip + 1, (0, 1)))
        return [
            remote(
                buffer.at[part, 2 * chip], buffer.at[part, slot],
                send.at[part, slot], recv.at[part, slot], row_off, col_off,
            )
            for slot, (row_off, col_off) in moves
        ]

    def poll(pack, part, slot):
        buffer, recv, send = pack

        @pl.when(slot > 0)
        def _():
            remote(
                buffer.at[part, slot], buffer.at[part, slot], send.at[0, 0], recv.at[part, slot], 0, 1
            ).wait_recv()

        for chip in range(1, chips):
            @pl.when(slot == 2 * chip)
            def _():
                for copy in forwards(pack, part, chip):
                    copy.start()

    def sent(pack, part):
        for chip in [0] + singles:
            own_copy(pack, part, chip).wait_send()
        for chip in range(1, chips):
            for copy in forwards(pack, part, chip):
                copy.wait_send()

    def plane_copy(part, t):
        return remote(
            vecs.at[part, 0], plane_vecs.at[part, t - 1],
            pvec_send.at[part, t - 1], pvec_recv.at[part, t - 1], *spread_over[t],
        )

    def column_sums(x):
        width = math.gcd(n, 128)
        folded = sum(x[:, s : s + width] for s in range(0, x.shape[1], width))
        return jnp.sum(folded.T, axis=0, keepdims=True)

    def spread(row):
        return jnp.broadcast_to(row, (probes, probes)).T

    def wide(row, width):
        return jnp.concatenate([spread(row)] * (width // probes), axis=1)

    def sum_copy(step, off):
        return remote(
            sums_out.at[step], sums_in.at[step, off], sum_send.at[step, off], sum_recv.at[step, off],
            off // cols, off % cols,
        )

    def give(step, squares, curvature):
        sums_out[step] = jnp.concatenate(
            [squares, curvature, jnp.zeros((6, probes), jnp.float32)], axis=0
        )
        for off in range(1, devices):
            sum_copy(step, off).start()

    def take(step):
        for off in range(1, devices):
            sum_copy(step, off).wait()
        result = tree_sum([sums_out[step]] + [sums_in[step, off] for off in range(1, devices)])
        sums_ref[step] = result
        squares, curvature = result[0:1], result[1:2]
        beta = jnp.sqrt(squares + epsilon)
        return curvature / (beta * beta), beta

    number, count = {}, 0
    for s in range(len(bits)):
        for u in range(plane >> (s + 1)):
            number[(s, u)] = count
            count += 1
    orders = [bits, bits[::-1]]

    def spots(h, s):
        done = sum(orders[h][: s + 1])
        return [u for u in range(plane) if not u & done]

    def reduce_copy(h, s, k):
        i = number[(s, k)]
        return remote(
            rs_out.at[h, i], rs_in.at[h, i], rs_send.at[h, i], rs_recv.at[h, i],
            *spread_over[orders[h][s]],
        )

    def received(h, s, t):
        k = spots(h, s).index(t)
        reduce_copy(h, s, k).wait_recv()
        return rs_in[h, number[(s, k)]].astype(jnp.float32)

    def reduce_stage(h, s, k):
        t = spots(h, s)[k] | orders[h][s]
        part = total[t, :, halves[h]]
        for earlier in range(s):
            part = part + received(h, earlier, t)
        rs_out[h, number[(s, k)]] = part.astype(jnp.bfloat16)
        reduce_copy(h, s, k).start()

    def reduce_rest(h):
        for s in range(1, len(bits)):
            for k in reversed(range(plane >> (s + 1))):
                reduce_stage(h, s, k)

    def reduced(h):
        value = total[0, :, halves[h]]
        for s in range(len(bits)):
            value = value + received(h, s, 0)
        return value

    def reduce_sent():
        for h in range(2):
            for s in range(len(bits)):
                for k in range(plane >> (s + 1)):
                    reduce_copy(h, s, k).wait_send()

    vec_pack = (vecs, vec_recv, vec_send)
    pts_pack = (points, pts_recv, pts_send)

    def send_own(h):
        for chip in reversed(singles):
            own_copy(vec_pack, h, chip).start()
        own_copy(vec_pack, h, 0).start()
        for t in range(1, plane):
            plane_copy(h, t).start()

    barrier = pltpu.get_barrier_semaphore()
    peers = [(r, c) for r in range(rows) for c in range(cols) if r or c]
    for peer in peers:
        pl.semaphore_signal(barrier, inc=1, device_id=device(*peer), device_id_type=MESH)

    dims = pts_ref.shape[0]
    index = lax.broadcasted_iota(jnp.int32, (dims, n), 0)
    scale = jnp.zeros((dims, n), jnp.float32)
    for d in range(dims):
        scale = jnp.where(index == d, scale_ref[d], scale)
    points[0, 0] = pts_ref[...] * scale * math.sqrt(math.log2(math.e))
    for s in range(0, n, 128):
        width = min(128, n)
        flipped = (2.0 * signs_ref[s : s + width, :].astype(jnp.float32) - 1.0).T
        start[:, s : s + width] = flipped.astype(jnp.bfloat16)
        vecs[s // half, 0, :, s % half : s % half + width] = flipped.astype(jnp.bfloat16)
    pl.semaphore_wait(barrier, len(peers))

    def plane_point_copy(t):
        return remote(
            points.at[0, 0], plane_points.at[t - 1], ppts_send.at[t - 1], ppts_recv.at[t - 1], *spread_over[t]
        )

    for t in range(1, plane):
        plane_point_copy(t).start()
    for chip in reversed(singles):
        own_copy(pts_pack, 0, chip).start()
    own_copy(pts_pack, 0, 0).start()
    for chip in singles[::-1] + [0]:
        for h in range(2):
            own_copy(vec_pack, h, chip).start()
    right[0] = features(points[0, 0], False).astype(jnp.bfloat16)
    for t in range(plane):
        total[t] = jnp.zeros((probes, n), jnp.float32)
    for t in range(1, plane):
        plane_point_copy(t).wait()
        right[t] = features(plane_points[t - 1], False).astype(jnp.bfloat16)

    def write(slot, h, c):
        return pltpu.make_async_copy(
            stage.at[2 * slot + h], far_ref.at[c, pl.ds(h * half, half)], write_sem.at[slot, h]
        )

    def read(slot, h, c):
        return pltpu.make_async_copy(
            far_ref.at[c, pl.ds(pl.multiple_of(h * half, half), half)], stage.at[slot], read_sem.at[slot]
        )

    def block(c, t, s, cut=slice(None)):
        if t == plane - 1:
            return stage.at[2 * lax.rem(c, 2) + s // half, s % half : s % half + tile, cut]
        return near.at[c, t, s : s + tile, cut]

    def vec(c, s):
        return vecs[s // half, c, :, s % half : s % half + tile]

    def first(c, forming, applying):
        slot = lax.rem(c, 2)
        order = [plane - 1] + list(range(plane - 1))
        if forming:
            poll(pts_pack, 0, c)
            left[...] = features(points[0, c], True).T.astype(jnp.bfloat16)
        if applying:
            for h in range(2):
                poll(vec_pack, h, c - 1)
                write(slot, h, c - 2).wait()
        for t in range(plane):
            parts = []
            for s in range(0, n, tile):
                if forming:
                    power = jnp.dot(
                        left[s : s + tile, :], right[t], preferred_element_type=jnp.float32
                    )
                    block(c, t, s)[...] = jnp.exp2(jnp.minimum(power, 0.0)).astype(jnp.bfloat16)
                if applying:
                    parts.append(jnp.dot(
                        vec(c - 2, s), block(c - 2, order[t], s)[...],
                        preferred_element_type=jnp.float32,
                    ))
            if applying:
                total[order[t]] += plain_sum(parts)
        if forming:
            for h in range(2):
                write(slot, h, c).start()

    def loop(low, high, forming, applying):
        def body(c, carry):
            first(c, forming, applying)
            return carry

        lax.fori_loop(low, high, body, 0)

    loop(0, 2, True, False)
    loop(2, slots, True, True)
    last = [slots - 2, slots - 1]
    for h in range(2):
        poll(vec_pack, h, slots - 1)
    for h in range(2):
        for t in reversed(range(plane)):
            parts = [
                jnp.dot(vec(c, s), block(c, t, s, halves[h])[...], preferred_element_type=jnp.float32)
                for c in last for s in range(0, n, tile)
            ]
            total[t, :, halves[h]] += plain_sum(parts)
            for k, u in enumerate(spots(h, 0)):
                if u | orders[h][0] == t:
                    reduce_stage(h, 0, k)
    for c in last:
        for h in range(2):
            write(c % 2, h, c).wait()
    for h in range(2):
        sent(vec_pack, h)
    sent(pts_pack, 0)
    for chip in [0] + singles:
        pl.semaphore_signal(
            free_sem, inc=1, device_id=device(*(gather[chip] if chip else (0, 1))), device_id_type=MESH
        )

    ring = 4

    def spot(i):
        turn = i // chips
        return turn % 2, turn // 2 * chips + i % chips

    for i in range(min(ring - 1, 2 * slots)):
        read(i, *spot(i)).start()

    both, cross, own = [], [], []
    for h in range(2):
        reduce_rest(h)
        value = reduced(h)
        now = start[:, halves[h]].astype(jnp.float32)
        image[:, halves[h]] = value
        vecs[h, 0] = (value - now).astype(jnp.bfloat16)
        if h == 0:
            pl.semaphore_wait(free_sem, 1 + len(singles))
        send_own(h)
        both.append(column_sums(now * value))
        cross.append(column_sums(value * (value - now)))
        own.append(column_sums(now * now))
    reduce_sent()
    both, cross, own = both[0] + both[1], cross[0] + cross[1], own[0] + own[1]
    give(0, own, both + noise_level * own)

    def product():
        def later(i, carry):
            h, c = spot(i)
            poll(vec_pack, h, c)
            slot = lax.rem(i, ring)

            @pl.when(i + ring - 1 < 2 * slots)
            def _():
                ahead = i + ring - 1
                read(lax.rem(ahead, ring), *spot(ahead)).start()

            for t in range(plane):
                if t == plane - 1:
                    read(slot, h, c).wait()
                    matrix = stage[slot]
                else:
                    matrix = near[c, t, pl.ds(pl.multiple_of(h * half, half), half), :]
                total[t] += jnp.dot(vecs[h, c], matrix, preferred_element_type=jnp.float32)
            return carry

        for t in range(plane):
            total[t] = jnp.zeros((probes, n), jnp.float32)
        lax.fori_loop(0, 2 * slots, later, 0)
        for h in range(2):
            sent(vec_pack, h)

    def plane_arrived():
        for h in range(2):
            for t in range(1, plane):
                plane_copy(h, t).wait()

    def plane_products(h):
        value = 0.0
        for t in range(1, plane):
            value = value + plane_vecs[h, t - 1].astype(jnp.float32) * total[t, :, halves[h]]
        return value

    product()
    plane_arrived()
    for k in reversed(range(plane // 2)):
        for h in range(2):
            reduce_stage(h, 0, k)
    for i in range(min(ring - 1, 2 * slots)):
        read(i, *spot(i)).start()
    alpha_1, beta_1 = take(0)
    shift = (1.0 + noise_level) - alpha_1
    inverse_1 = 1.0 / beta_1
    shift_half, inverse_half = wide(shift, half), wide(inverse_1, half)
    square, form = 0.0, 0.0
    for h in range(2):
        span = halves[h]
        now = start[:, span].astype(jnp.float32)
        excess = image[:, span] - now
        fresh = (excess + shift_half * now) * inverse_half
        square = square + column_sums(fresh * fresh)
        form = form + column_sums(excess * total[0, :, span] + plane_products(h))
    form = (form + 2.0 * shift * cross + shift * shift * both) * inverse_1 * inverse_1
    give(1, square, form + noise_level * square)
    for h in range(2):
        reduce_rest(h)
    alpha_2, beta_2 = take(1)
    inverse_2 = 1.0 / beta_2
    scale_now = wide(inverse_2 * inverse_1, half)
    minus, back = wide(alpha_2 * inverse_2, half), wide(beta_2 * inverse_1, half)
    square = 0.0
    for h in range(2):
        span = halves[h]
        now, old = start[:, span].astype(jnp.float32), image[:, span]
        value = (reduced(h) + shift_half * old) * scale_now
        direction = (old - now + shift_half * now) * inverse_half
        value = value + (noise_level * wide(inverse_2, half) - minus) * direction - back * now
        vecs[h, 0] = value.astype(jnp.bfloat16)
        send_own(h)
        image[:, span] = value
        square = square + column_sums(value * value)
    reduce_sent()

    product()
    plane_arrived()
    form = 0.0
    for h in range(2):
        span = halves[h]
        form = form + column_sums(image[:, span] * total[0, :, span] + plane_products(h))
    give(2, square, form + noise_level * square)
    take(2)


def log_weight(alpha_list, beta_list):
    degree = len(alpha_list)
    width_probes = alpha_list[0].shape[0]
    zeros_row = jnp.zeros((width_probes,), jnp.float32)
    ones_row = jnp.ones((width_probes,), jnp.float32)
    matrix = []
    vectors = []
    for first_idx in range(degree):
        entries = []
        basis_row = []
        for second_idx in range(degree):
            if first_idx == second_idx:
                entries.append(alpha_list[first_idx])
                basis_row.append(ones_row)
            elif abs(first_idx - second_idx) == 1:
                entries.append(beta_list[min(first_idx, second_idx)])
                basis_row.append(zeros_row)
            else:
                entries.append(zeros_row)
                basis_row.append(zeros_row)
        matrix.append(entries)
        vectors.append(basis_row)
    for sweep_index in range(jacobi_sweeps):
        for first_idx in range(degree):
            for second_idx in range(first_idx + 1, degree):
                coupling = matrix[first_idx][second_idx]
                rotate_by = 0.5 * jnp.arctan2(
                    2.0 * coupling, matrix[second_idx][second_idx] - matrix[first_idx][first_idx]
                )
                cosine = jnp.cos(rotate_by)
                sine_val = jnp.sin(rotate_by)
                for row_idx in range(degree):
                    left_val = matrix[row_idx][first_idx]
                    right_val = matrix[row_idx][second_idx]
                    matrix[row_idx][first_idx] = cosine * left_val - sine_val * right_val
                    matrix[row_idx][second_idx] = sine_val * left_val + cosine * right_val
                    left_vec = vectors[row_idx][first_idx]
                    right_vec = vectors[row_idx][second_idx]
                    vectors[row_idx][first_idx] = cosine * left_vec - sine_val * right_vec
                    vectors[row_idx][second_idx] = sine_val * left_vec + cosine * right_vec
                for col_idx in range(degree):
                    upper_val = matrix[first_idx][col_idx]
                    lower_val = matrix[second_idx][col_idx]
                    matrix[first_idx][col_idx] = cosine * upper_val - sine_val * lower_val
                    matrix[second_idx][col_idx] = sine_val * upper_val + cosine * lower_val
    total = zeros_row
    for index_k in range(degree):
        total = total + vectors[0][index_k] * vectors[0][index_k] * jnp.log(
            matrix[index_k][index_k]
        )
    return total


def per_device(rows, cols, points, inverse_scales, probe_signs):
    dims, n = points.shape
    probes = probe_signs.shape[1]
    slots, plane, devices = 2 * len(groups(rows, cols)[0]), len(groups(rows, cols)[1]), rows * cols
    dma = pltpu.SemaphoreType.DMA
    vmem = pltpu.VMEM
    sums, _ = pl.pallas_call(
        functools.partial(kernel, rows, cols),
        out_shape=(
            jax.ShapeDtypeStruct((STEPS, 8, probes), jnp.float32),
            jax.ShapeDtypeStruct((slots, n, n), jnp.bfloat16),
        ),
        in_specs=[
            pl.BlockSpec(memory_space=pltpu.VMEM),
            pl.BlockSpec(memory_space=pltpu.SMEM),
            pl.BlockSpec(memory_space=pltpu.VMEM),
        ],
        out_specs=(
            pl.BlockSpec(memory_space=pltpu.VMEM),
            pl.BlockSpec(memory_space=pl.ANY),
        ),
        scratch_shapes=[
            vmem((slots, plane - 1, n, n), jnp.bfloat16),
            vmem((4, n // 2, n), jnp.bfloat16),
            vmem((2, slots, probes, n // 2), jnp.bfloat16),
            vmem((1, slots, dims, n), jnp.float32),
            vmem((plane - 1, dims, n), jnp.float32),
            vmem((2, plane - 1, probes, n // 2), jnp.bfloat16),
            vmem((n, 8 * dims), jnp.bfloat16),
            vmem((plane, 8 * dims, n), jnp.bfloat16),
            vmem((plane, probes, n), jnp.float32),
            vmem((probes, n), jnp.bfloat16),
            vmem((probes, n), jnp.float32),
            vmem((2, plane - 1, probes, n // 2), jnp.bfloat16),
            vmem((2, plane - 1, probes, n // 2), jnp.bfloat16),
            vmem((STEPS, 8, probes), jnp.float32),
            vmem((STEPS, devices, 8, probes), jnp.float32),
            dma((1, slots)),
            dma((1, slots)),
            dma((2, slots)),
            dma((2, slots)),
            dma((plane - 1,)),
            dma((plane - 1,)),
            dma((2, plane - 1)),
            dma((2, plane - 1)),
            dma((2, plane - 1)),
            dma((2, plane - 1)),
            dma((2, 2)),
            dma((4,)),
            dma((STEPS, devices)),
            dma((STEPS, devices)),
            pltpu.SemaphoreType.REGULAR,
        ],
        compiler_params=pltpu.CompilerParams(
            collective_id=0, has_side_effects=True, vmem_limit_bytes=64 * 2**20 - 65536
        ),
        name="lanczos",
    )(points, inverse_scales, probe_signs)
    beta_list = [jnp.sqrt(sums[k, 0] + epsilon) for k in range(STEPS)]
    alpha_list = [sums[k, 1] / (beta_list[k] * beta_list[k]) for k in range(STEPS)]
    return alpha_list[0], log_weight(alpha_list, beta_list[1:])


def solution(mesh):
    in_specs = (P(None, ("row", "col")), P(), P(("row", "col"), None))
    out_specs = (P(), P())
    return jax.shard_map(
        functools.partial(per_device, mesh.shape["row"], mesh.shape["col"]),
        mesh=mesh, in_specs=in_specs, out_specs=out_specs, check_vma=False,
    )
```

```python
import functools
import math

import jax
import jax.numpy as jnp
from jax import lax
from jax.experimental import pallas as pl
from jax.experimental.pallas import tpu as pltpu
from jax.sharding import PartitionSpec as P

STEPS = 3


epsilon = 1e-06
noise_level = 1.0
jacobi_sweeps = 6
MESH = pl.DeviceIdType.MESH


def flip(index, mask):
    bit = 1
    out = index
    while bit <= mask:
        if mask & bit:
            out = out + bit * (1 - 2 * ((index // bit) % 2))
        bit *= 2
    return out


def bits_below(count):
    return [1 << k for k in range(16) if (1 << k) < count]


def three_parts(x):
    high = x.astype(jnp.bfloat16).astype(jnp.float32)
    rest = x - high
    middle = rest.astype(jnp.bfloat16).astype(jnp.float32)
    low = (rest - middle).astype(jnp.bfloat16).astype(jnp.float32)
    return high, middle, low


def features(x, left):
    high, middle, low = three_parts(x)
    norm = -0.5 * jnp.sum(x * x, axis=0, keepdims=True)
    parts = three_parts(norm)
    rows = lax.broadcasted_iota(jnp.int32, x.shape, 0)
    first = 0 if left else 3
    ones_at = 3 if left else 0
    tail = jnp.where((rows >= ones_at) & (rows < ones_at + 3), 1.0, 0.0)
    for k in range(3):
        tail = jnp.where(rows == first + k, parts[k], tail)
    blank = jnp.zeros_like(x)
    if left:
        groups = [high, high, middle, middle, high, low, tail, blank]
    else:
        groups = [high, middle, high, middle, low, high, tail, blank]
    return jnp.concatenate(groups, axis=0)


def tree_sum(values):
    while len(values) > 1:
        values = [values[k] + values[k + 1] for k in range(0, len(values), 2)]
    return values[0]


def plain_sum(values):
    result = values[0]
    for value in values[1:]:
        result = result + value
    return result


def groups(rows, cols):
    gather = [(1 << k, 0) for k in range(16) if (1 << k) < rows]
    other = [(0, 1 << k) for k in range(1, 16) if (1 << k) < cols]

    def offsets(bits):
        table = [(0, 0)]
        for row_off, col_off in bits:
            table += [(r + row_off, c + col_off) for r, c in table]
        return table

    return offsets(gather), offsets(other)


def kernel(
    rows, cols,
    pts_ref, scale_ref, signs_ref,
    sums_ref, far_ref,
    near, stage, vecs, points, plane_points, plane_vecs, left, right, total, start, image,
    rs_out, rs_in, sums_out, sums_in,
    pts_recv, pts_send, vec_recv, vec_send, ppts_recv, ppts_send, pvec_recv, pvec_send,
    rs_recv, rs_send, write_sem, read_sem, sum_recv, sum_send, free_sem,
):
    gather, spread_over = groups(rows, cols)
    slots, plane, devices = 2 * len(gather), len(spread_over), rows * cols
    n, probes = pts_ref.shape[1], signs_ref.shape[1]
    my_row, my_col = lax.axis_index("row"), lax.axis_index("col")
    half = n // 2
    tile = math.gcd(half, 256)
    halves = [slice(h * half, (h + 1) * half) for h in range(2)]
    bits = bits_below(plane)

    def device(row_off, col_off):
        return (flip(my_row, row_off), flip(my_col, col_off))

    def remote(src, dst, send_sem, recv_sem, row_off, col_off):
        return pltpu.make_async_remote_copy(
            src_ref=src, dst_ref=dst, send_sem=send_sem, recv_sem=recv_sem,
            device_id=device(row_off, col_off), device_id_type=MESH,
        )

    chips = slots // 2
    singles = bits_below(chips)

    def own_copy(pack, part, chip):
        buffer, recv, send = pack
        slot = 2 * chip if chip else 1
        row_off, col_off = gather[chip] if chip else (0, 1)
        return remote(
            buffer.at[part, 0], buffer.at[part, slot], send.at[part, chip], recv.at[part, slot],
            row_off, col_off,
        )

    def forwards(pack, part, chip):
        buffer, recv, send = pack
        low = chip & -chip
        moves = [(2 * (chip | bit), gather[bit]) for bit in singles if bit < low]
        moves.append((2 * chip + 1, (0, 1)))
        return [
            remote(
                buffer.at[part, 2 * chip], buffer.at[part, slot],
                send.at[part, slot], recv.at[part, slot], row_off, col_off,
            )
            for slot, (row_off, col_off) in moves
        ]

    def poll(pack, part, slot):
        buffer, recv, send = pack

        @pl.when(slot > 0)
        def _():
            remote(
                buffer.at[part, slot], buffer.at[part, slot], send.at[0, 0], recv.at[part, slot], 0, 1
            ).wait_recv()

        for chip in range(1, chips):
            @pl.when(slot == 2 * chip)
            def _():
                for copy in forwards(pack, part, chip):
                    copy.start()

    def sent(pack, part):
        for chip in [0] + singles:
            own_copy(pack, part, chip).wait_send()
        for chip in range(1, chips):
            for copy in forwards(pack, part, chip):
                copy.wait_send()

    def plane_copy(part, t):
        return remote(
            vecs.at[part, 0], plane_vecs.at[part, t - 1],
            pvec_send.at[part, t - 1], pvec_recv.at[part, t - 1], *spread_over[t],
        )

    def column_sums(x):
        width = math.gcd(n, 128)
        folded = sum(x[:, s : s + width] for s in range(0, x.shape[1], width))
        return jnp.sum(folded.T, axis=0, keepdims=True)

    def spread(row):
        return jnp.broadcast_to(row, (probes, probes)).T

    def wide(row, width):
        return jnp.concatenate([spread(row)] * (width // probes), axis=1)

    def sum_copy(step, off):
        return remote(
            sums_out.at[step], sums_in.at[step, off], sum_send.at[step, off], sum_recv.at[step, off],
            off // cols, off % cols,
        )

    def give(step, squares, curvature):
        sums_out[step] = jnp.concatenate([squares, curvature], axis=0)
        for off in range(1, devices):
            sum_copy(step, off).start()

    def take(step):
        for off in range(1, devices):
            sum_copy(step, off).wait()
        result = tree_sum([sums_out[step]] + [sums_in[step, off] for off in range(1, devices)])
        sums_ref[step, 0:2] = result
        squares, curvature = result[0:1], result[1:2]
        beta = jnp.sqrt(squares + epsilon)
        return curvature / (beta * beta), beta

    number, count = {}, 0
    for s in range(len(bits)):
        for u in range(plane >> (s + 1)):
            number[(s, u)] = count
            count += 1
    orders = [bits, bits[::-1]]

    def spots(h, s):
        done = sum(orders[h][: s + 1])
        return [u for u in range(plane) if not u & done]

    def reduce_copy(h, s, k):
        i = number[(s, k)]
        return remote(
            rs_out.at[h, i], rs_in.at[h, i], rs_send.at[h, i], rs_recv.at[h, i],
            *spread_over[orders[h][s]],
        )

    def received(h, s, t):
        k = spots(h, s).index(t)
        reduce_copy(h, s, k).wait_recv()
        return rs_in[h, number[(s, k)]].astype(jnp.float32)

    def reduce_stage(h, s, k):
        t = spots(h, s)[k] | orders[h][s]
        part = total[t, :, halves[h]]
        for earlier in range(s):
            part = part + received(h, earlier, t)
        rs_out[h, number[(s, k)]] = part.astype(jnp.bfloat16)
        reduce_copy(h, s, k).start()

    def reduce_rest(h):
        for s in range(1, len(bits)):
            for k in reversed(range(plane >> (s + 1))):
                reduce_stage(h, s, k)

    def reduced(h):
        value = total[0, :, halves[h]]
        for s in range(len(bits)):
            value = value + received(h, s, 0)
        return value

    def reduce_sent():
        for h in range(2):
            for s in range(len(bits)):
                for k in range(plane >> (s + 1)):
                    reduce_copy(h, s, k).wait_send()

    vec_pack = (vecs, vec_recv, vec_send)
    pts_pack = (points, pts_recv, pts_send)

    def send_own(h):
        for chip in reversed(singles):
            own_copy(vec_pack, h, chip).start()
        own_copy(vec_pack, h, 0).start()

    def send_plane():
        for t in range(1, plane):
            for h in range(2):
                plane_copy(h, t).start()

    barrier = pltpu.get_barrier_semaphore()
    peers = [(r, c) for r in range(rows) for c in range(cols) if r or c]
    for peer in peers:
        pl.semaphore_signal(barrier, inc=1, device_id=device(*peer), device_id_type=MESH)

    dims = pts_ref.shape[0]
    index = lax.broadcasted_iota(jnp.int32, (dims, n), 0)
    scale = jnp.zeros((dims, n), jnp.float32)
    for d in range(dims):
        scale = jnp.where(index == d, scale_ref[d], scale)
    points[0, 0] = pts_ref[...] * scale * math.sqrt(math.log2(math.e))
    for s in range(0, n, 128):
        width = min(128, n)
        flipped = (2.0 * signs_ref[s : s + width, :].astype(jnp.float32) - 1.0).T
        start[:, s : s + width] = flipped.astype(jnp.bfloat16)
        vecs[s // half, 0, :, s % half : s % half + width] = flipped.astype(jnp.bfloat16)
    pl.semaphore_wait(barrier, len(peers))

    def plane_point_copy(t):
        return remote(
            points.at[0, 0], plane_points.at[t - 1], ppts_send.at[t - 1], ppts_recv.at[t - 1], *spread_over[t]
        )

    for t in range(1, plane):
        plane_point_copy(t).start()
    for chip in reversed(singles):
        own_copy(pts_pack, 0, chip).start()
    own_copy(pts_pack, 0, 0).start()
    for chip in singles[::-1] + [0]:
        for h in range(2):
            own_copy(vec_pack, h, chip).start()
    right[0] = features(points[0, 0], False).astype(jnp.bfloat16)
    for t in range(plane):
        total[t] = jnp.zeros((probes, n), jnp.float32)
    for t in range(1, plane):
        plane_point_copy(t).wait()
        right[t] = features(plane_points[t - 1], False).astype(jnp.bfloat16)

    def write(slot, h, c):
        return pltpu.make_async_copy(
            stage.at[2 * slot + h], far_ref.at[c, pl.ds(h * half, half)], write_sem.at[slot, h]
        )

    def read(slot, h, c):
        return pltpu.make_async_copy(
            far_ref.at[c, pl.ds(pl.multiple_of(h * half, half), half)], stage.at[slot], read_sem.at[slot]
        )

    def block(c, t, s, cut=slice(None)):
        if t == plane - 1:
            return stage.at[2 * lax.rem(c, 2) + s // half, s % half : s % half + tile, cut]
        return near.at[c, t, s : s + tile, cut]

    def vec(c, s):
        return vecs[s // half, c, :, s % half : s % half + tile]

    def first(c, forming, applying):
        slot = lax.rem(c, 2)
        order = [plane - 1] + list(range(plane - 1))
        if forming:
            poll(pts_pack, 0, c)
            left[...] = features(points[0, c], True).T.astype(jnp.bfloat16)
        if applying:
            for h in range(2):
                poll(vec_pack, h, c - 1)
                write(slot, h, c - 2).wait()
        for t in range(plane):
            parts = []
            for s in range(0, n, tile):
                if forming:
                    power = jnp.dot(
                        left[s : s + tile, :], right[t], preferred_element_type=jnp.float32
                    )
                    block(c, t, s)[...] = jnp.exp2(jnp.minimum(power, 0.0)).astype(jnp.bfloat16)
                if applying:
                    parts.append(jnp.dot(
                        vec(c - 2, s), block(c - 2, order[t], s)[...],
                        preferred_element_type=jnp.float32,
                    ))
            if applying:
                total[order[t]] += plain_sum(parts)
        if forming:
            for h in range(2):
                write(slot, h, c).start()

    def loop(low, high, forming, applying):
        def body(c, carry):
            first(c, forming, applying)
            return carry

        lax.fori_loop(low, high, body, 0)

    loop(0, 2, True, False)
    loop(2, slots, True, True)
    last = [slots - 2, slots - 1]
    for h in range(2):
        poll(vec_pack, h, slots - 1)
    for h in range(2):
        for t in reversed(range(plane)):
            parts = [
                jnp.dot(vec(c, s), block(c, t, s, halves[h])[...], preferred_element_type=jnp.float32)
                for c in last for s in range(0, n, tile)
            ]
            total[t, :, halves[h]] += plain_sum(parts)
            for k, u in enumerate(spots(h, 0)):
                if u | orders[h][0] == t:
                    reduce_stage(h, 0, k)
    for c in last:
        for h in range(2):
            write(c % 2, h, c).wait()
    for h in range(2):
        sent(vec_pack, h)
    sent(pts_pack, 0)
    for chip in [0] + singles:
        pl.semaphore_signal(
            free_sem, inc=1, device_id=device(*(gather[chip] if chip else (0, 1))), device_id_type=MESH
        )

    ring = 4

    def spot(i):
        turn = i // chips
        return turn % 2, turn // 2 * chips + i % chips

    for i in range(min(ring - 1, 2 * slots)):
        read(i, *spot(i)).start()

    both, cross, own = [], [], []
    for h in range(2):
        reduce_rest(h)
    for h in range(2):
        value = reduced(h)
        now = start[:, halves[h]].astype(jnp.float32)
        image[:, halves[h]] = value
        vecs[h, 0] = (value - now).astype(jnp.bfloat16)
        if h == 0:
            pl.semaphore_wait(free_sem, 1 + len(singles))
        send_own(h)
        both.append(column_sums(now * value))
        cross.append(column_sums(value * (value - now)))
        own.append(column_sums(now * now))
    send_plane()
    reduce_sent()
    both, cross, own = both[0] + both[1], cross[0] + cross[1], own[0] + own[1]
    give(0, own, both + noise_level * own)

    def product():
        def later(i, carry):
            h, c = spot(i)
            poll(vec_pack, h, c)
            slot = lax.rem(i, ring)

            @pl.when(i + ring - 1 < 2 * slots)
            def _():
                ahead = i + ring - 1
                read(lax.rem(ahead, ring), *spot(ahead)).start()

            for t in range(plane):
                if t == plane - 1:
                    read(slot, h, c).wait()
                    matrix = stage[slot]
                else:
                    matrix = near[c, t, pl.ds(pl.multiple_of(h * half, half), half), :]
                total[t] += jnp.dot(vecs[h, c], matrix, preferred_element_type=jnp.float32)
            return carry

        for t in range(plane):
            total[t] = jnp.zeros((probes, n), jnp.float32)
        def two(j, carry):
            return later(2 * j + 1, later(2 * j, carry))

        lax.fori_loop(0, slots, two, 0)
        for h in range(2):
            sent(vec_pack, h)

    def plane_arrived():
        for h in range(2):
            for t in range(1, plane):
                plane_copy(h, t).wait()

    def plane_products(h):
        value = 0.0
        for t in range(1, plane):
            value = value + plane_vecs[h, t - 1].astype(jnp.float32) * total[t, :, halves[h]]
        return value

    product()
    plane_arrived()
    for k in reversed(range(plane // 2)):
        for h in range(2):
            reduce_stage(h, 0, k)
    for i in range(min(ring - 1, 2 * slots)):
        read(i, *spot(i)).start()
    alpha_1, beta_1 = take(0)
    shift = (1.0 + noise_level) - alpha_1
    inverse_1 = 1.0 / beta_1
    shift_half, inverse_half = wide(shift, half), wide(inverse_1, half)
    square, form = 0.0, 0.0
    for h in range(2):
        span = halves[h]
        now = start[:, span].astype(jnp.float32)
        excess = image[:, span] - now
        fresh = (excess + shift_half * now) * inverse_half
        square = square + column_sums(fresh * fresh)
        form = form + column_sums(excess * total[0, :, span] + plane_products(h))
    form = (form + 2.0 * shift * cross + shift * shift * both) * inverse_1 * inverse_1
    give(1, square, form + noise_level * square)
    for h in range(2):
        reduce_rest(h)
    alpha_2, beta_2 = take(1)
    inverse_2 = 1.0 / beta_2
    scale_now = wide(inverse_2 * inverse_1, half)
    minus, back = wide(alpha_2 * inverse_2, half), wide(beta_2 * inverse_1, half)
    square = 0.0
    for h in range(2):
        span = halves[h]
        now, old = start[:, span].astype(jnp.float32), image[:, span]
        value = (reduced(h) + shift_half * old) * scale_now
        direction = (old - now + shift_half * now) * inverse_half
        value = value + (noise_level * wide(inverse_2, half) - minus) * direction - back * now
        vecs[h, 0] = value.astype(jnp.bfloat16)
        send_own(h)
        image[:, span] = value
        square = square + column_sums(value * value)
    send_plane()
    reduce_sent()

    product()
    plane_arrived()
    form = 0.0
    for h in range(2):
        span = halves[h]
        form = form + column_sums(image[:, span] * total[0, :, span] + plane_products(h))
    give(2, square, form + noise_level * square)
    take(2)


def log_weight(alpha_list, beta_list):
    degree = len(alpha_list)
    width_probes = alpha_list[0].shape[0]
    zeros_row = jnp.zeros((width_probes,), jnp.float32)
    ones_row = jnp.ones((width_probes,), jnp.float32)
    matrix = []
    vectors = []
    for first_idx in range(degree):
        entries = []
        basis_row = []
        for second_idx in range(degree):
            if first_idx == second_idx:
                entries.append(alpha_list[first_idx])
                basis_row.append(ones_row)
            elif abs(first_idx - second_idx) == 1:
                entries.append(beta_list[min(first_idx, second_idx)])
                basis_row.append(zeros_row)
            else:
                entries.append(zeros_row)
                basis_row.append(zeros_row)
        matrix.append(entries)
        vectors.append(basis_row)
    for sweep_index in range(jacobi_sweeps):
        for first_idx in range(degree):
            for second_idx in range(first_idx + 1, degree):
                coupling = matrix[first_idx][second_idx]
                rotate_by = 0.5 * jnp.arctan2(
                    2.0 * coupling, matrix[second_idx][second_idx] - matrix[first_idx][first_idx]
                )
                cosine = jnp.cos(rotate_by)
                sine_val = jnp.sin(rotate_by)
                for row_idx in range(degree):
                    left_val = matrix[row_idx][first_idx]
                    right_val = matrix[row_idx][second_idx]
                    matrix[row_idx][first_idx] = cosine * left_val - sine_val * right_val
                    matrix[row_idx][second_idx] = sine_val * left_val + cosine * right_val
                    left_vec = vectors[row_idx][first_idx]
                    right_vec = vectors[row_idx][second_idx]
                    vectors[row_idx][first_idx] = cosine * left_vec - sine_val * right_vec
                    vectors[row_idx][second_idx] = sine_val * left_vec + cosine * right_vec
                for col_idx in range(degree):
                    upper_val = matrix[first_idx][col_idx]
                    lower_val = matrix[second_idx][col_idx]
                    matrix[first_idx][col_idx] = cosine * upper_val - sine_val * lower_val
                    matrix[second_idx][col_idx] = sine_val * upper_val + cosine * lower_val
    total = zeros_row
    for index_k in range(degree):
        total = total + vectors[0][index_k] * vectors[0][index_k] * jnp.log(
            matrix[index_k][index_k]
        )
    return total


def per_device(rows, cols, points, inverse_scales, probe_signs):
    dims, n = points.shape
    probes = probe_signs.shape[1]
    slots, plane, devices = 2 * len(groups(rows, cols)[0]), len(groups(rows, cols)[1]), rows * cols
    dma = pltpu.SemaphoreType.DMA
    vmem = pltpu.VMEM
    sums, _ = pl.pallas_call(
        functools.partial(kernel, rows, cols),
        out_shape=(
            jax.ShapeDtypeStruct((STEPS, 8, probes), jnp.float32),
            jax.ShapeDtypeStruct((slots, n, n), jnp.bfloat16),
        ),
        in_specs=[
            pl.BlockSpec(memory_space=pltpu.VMEM),
            pl.BlockSpec(memory_space=pltpu.SMEM),
            pl.BlockSpec(memory_space=pltpu.VMEM),
        ],
        out_specs=(
            pl.BlockSpec(memory_space=pltpu.VMEM),
            pl.BlockSpec(memory_space=pl.ANY),
        ),
        scratch_shapes=[
            vmem((slots, plane - 1, n, n), jnp.bfloat16),
            vmem((4, n // 2, n), jnp.bfloat16),
            vmem((2, slots, probes, n // 2), jnp.bfloat16),
            vmem((1, slots, dims, n), jnp.float32),
            vmem((plane - 1, dims, n), jnp.float32),
            vmem((2, plane - 1, probes, n // 2), jnp.bfloat16),
            vmem((n, 8 * dims), jnp.bfloat16),
            vmem((plane, 8 * dims, n), jnp.bfloat16),
            vmem((plane, probes, n), jnp.float32),
            vmem((probes, n), jnp.bfloat16),
            vmem((probes, n), jnp.float32),
            vmem((2, plane - 1, probes, n // 2), jnp.bfloat16),
            vmem((2, plane - 1, probes, n // 2), jnp.bfloat16),
            vmem((STEPS, 2, probes), jnp.float32),
            vmem((STEPS, devices, 2, probes), jnp.float32),
            dma((1, slots)),
            dma((1, slots)),
            dma((2, slots)),
            dma((2, slots)),
            dma((plane - 1,)),
            dma((plane - 1,)),
            dma((2, plane - 1)),
            dma((2, plane - 1)),
            dma((2, plane - 1)),
            dma((2, plane - 1)),
            dma((2, 2)),
            dma((4,)),
            dma((STEPS, devices)),
            dma((STEPS, devices)),
            pltpu.SemaphoreType.REGULAR,
        ],
        compiler_params=pltpu.CompilerParams(
            collective_id=0, has_side_effects=True, vmem_limit_bytes=64 * 2**20 - 65536
        ),
        name="lanczos",
    )(points, inverse_scales, probe_signs)
    beta_list = [jnp.sqrt(sums[k, 0] + epsilon) for k in range(STEPS)]
    alpha_list = [sums[k, 1] / (beta_list[k] * beta_list[k]) for k in range(STEPS)]
    return alpha_list[0], log_weight(alpha_list, beta_list[1:])


def solution(mesh):
    in_specs = (P(None, ("row", "col")), P(), P(("row", "col"), None))
    out_specs = (P(), P())
    return jax.shard_map(
        functools.partial(per_device, mesh.shape["row"], mesh.shape["col"]),
        mesh=mesh, in_specs=in_specs, out_specs=out_specs, check_vma=False,
    )
```
